128 devices in a mesh: pair: 8 (over x, core), aux: 16 (over y, z).
Axes of the slice: x: 4, y: 4, z: 4, core: 2. Of those that a mesh axis runs over, the one named last changes fastest.
Arguments:
- left_active: bfloat16 [80, 128, 61440], P('pair', None, 'aux'), may hold values from -0.375 to 0.375
- right_active: bfloat16 [80, 128, 61440], P('pair', None, 'aux'), may hold values from -0.375 to 0.375
- amps_active: bfloat16 [80, 128, 128], P('pair', 'aux'), may hold values from -0.5 to 0.5
- rank_active: int32 [80], P('pair'), may hold values from 80 to 128, as said below
- gap_active: float32 [80], P('pair'), may hold values from 0.5 to 2
- energy_active: float32 [80, 128], P('pair'), may hold values from 0.5 to 4
- intersect_active: bfloat16 [80, 4, 128, 128], P('pair'), may hold values from -0.75 to 0.75
- fock_active: float32 [80, 4], P('pair'), may hold values from -2 to 2
- neighbor_active: int32 [80, 4], P('pair'), may hold values from 0 to 79
- left_env: bfloat16 [32, 48, 61440], P('pair', None, 'aux'), may hold values from -0.375 to 0.375
- right_env: bfloat16 [32, 48, 61440], P('pair', None, 'aux'), may hold values from -0.375 to 0.375
- amps_env: bfloat16 [32, 48, 48], P('pair', 'aux'), may hold values from -0.875 to 0.875
- rank_env: int32 [32], P('pair'), may hold values from 24 to 48, as said below
- gap_env: float32 [32], P('pair'), may hold values from 0.5 to 2
- energy_env: float32 [32, 48], P('pair'), may hold values from 0.5 to 4
- intersect_env: bfloat16 [32, 4, 48, 48], P('pair'), may hold values from -1.25 to 1.25
- fock_env: float32 [32, 4], P('pair'), may hold values from -2 to 2
- neighbor_env: int32 [32, 4], P('pair'), may hold values from 0 to 31
Outputs:
- new_active: float32 [80, 128, 128], P('pair', 'aux')
- new_env: float32 [32, 48, 48], P('pair', 'aux')
The draws below stay inside these ranges and needn't reach their ends.
Inputs may be any that keep to these rules, and one draw needn't show every extreme that they name: `rank_active`: multiples of 8; the first active pair has rank 128. `rank_env`: multiples of 8; the first environment pair has rank 48.
All inputs are finite; a program needn't handle non-finite values.
Results may differ from the reference program's by a relative error of at most 0.0041.
Values may be sent and summed in bfloat16 or wider, within the bound.
No kernel may reach another device: no remote copies, remote signals or barrier semaphores. Data moves between devices by JAX's collectives and lax.ppermute only.
A program may use at most 128 MiB of HBM per device.

```python
import math
import jax
import jax.numpy as jnp
from jax import lax

RA = 128
RE = 48
NAUX = 61440
NB = 4
PA = 80
PE = 32


def draw_rank_active(key, part):
    values = 8 * jax.random.randint(key, (PA,), RA * 5 // 64, RA // 8 + 1)
    return values.at[0].set(RA).astype(jnp.int32)


def draw_rank_env(key, part):
    values = 8 * jax.random.randint(key, (PE,), RE // 16, RE // 8 + 1)
    return values.at[0].set(RE).astype(jnp.int32)


def set_ends(array, key, least, high):
    longest = array.shape.index(max(array.shape))
    spots = []
    for shift in (0, 1):
        where = [jax.random.randint(jax.random.fold_in(key, axis), (), 0, length) for axis, length in enumerate(array.shape)]
        where[longest] = (where[longest] + shift) % array.shape[longest]
        spots.append(tuple(where))
    return array.at[spots[0]].set(least).at[spots[1]].set(high)


def block_scale(own_key, extent, shards, least, largest):
    factor_of = 1.0
    for position, blocks in shards:
        steps = jax.random.uniform(jax.random.fold_in(jax.random.fold_in(own_key, 6), position), (blocks,), jnp.float32, least / len(shards), largest / len(shards))
        factor_of = factor_of * jnp.repeat(jnp.exp(steps), extent[position] // blocks).reshape((-1,) + (1,) * (len(extent) - 1 - position))
    return factor_of


def normal_values(own_key, dims, width, most, pieces=(), held_as=jnp.bfloat16):
    factor_of = block_scale(own_key, dims, pieces, -0.22, 0.18) if pieces else 1.0
    entries = jax.random.normal(own_key, dims, jnp.float32) * width * factor_of
    return jnp.minimum(jnp.maximum(entries, -most), most).astype(held_as)


def setup_inputs(seed: int = 0) -> dict:
    key_list = jax.random.split(jax.random.key(seed), 19)
    left_active = normal_values(key_list[0], (PA, RA, NAUX), (NAUX ** -0.25), 0.375, ((0, 8), (2, 16)))
    right_active = normal_values(key_list[1], (PA, RA, NAUX), (NAUX ** -0.25), 0.375, ((0, 8), (2, 16)))
    amps_active = normal_values(key_list[2], (PA, RA, RA), (RA ** -0.5), 0.5, ((0, 8), (1, 16)))
    rank_active = draw_rank_active(jax.random.fold_in(key_list[18], 71), 0)
    gap_active = jnp.clip(jnp.exp(math.log(2.0) - 1.3862944 * jax.random.uniform(key_list[4], (PA,), jnp.float32) ** block_scale(key_list[4], (PA,), ((0, 8),), -0.2, 0.2)), 0.5, 2.0)
    energy_active = jnp.clip(jnp.exp(math.log(4.0) - 2.0794415 * jax.random.uniform(key_list[5], (PA, RA), jnp.float32) ** block_scale(key_list[5], (PA, RA), ((0, 8),), -0.2, 0.2)), 0.5, 4.0)
    intersect_active = normal_values(key_list[6], (PA, NB, RA, RA), (RA // 2) ** -0.5, 0.75, ((0, 8),))
    fock_active = jnp.clip(jax.random.uniform(key_list[7], (PA, NB), jnp.float32, -2.0, 2.0) * block_scale(key_list[7], (PA, NB), ((0, 8),), -0.4, 0.0), -2.0, 2.0)
    neighbor_active = set_ends(jax.random.randint(key_list[8], (PA, NB), 0, PA), jax.random.fold_in(key_list[8], 1), 0, PA - 1).astype(jnp.int32)
    left_env = normal_values(key_list[9], (PE, RE, NAUX), (NAUX ** -0.25), 0.375, ((0, 8), (2, 16)))
    right_env = normal_values(key_list[10], (PE, RE, NAUX), (NAUX ** -0.25), 0.375, ((0, 8), (2, 16)))
    amps_env = normal_values(key_list[11], (PE, RE, RE), (RE ** -0.5), 0.875, ((0, 8), (1, 16)))
    rank_env = draw_rank_env(jax.random.fold_in(key_list[18], 71), 0)
    gap_env = jnp.clip(jnp.exp(math.log(2.0) - 1.3862944 * jax.random.uniform(key_list[13], (PE,), jnp.float32) ** block_scale(key_list[13], (PE,), ((0, 8),), -0.2, 0.2)), 0.5, 2.0)
    energy_env = jnp.clip(jnp.exp(math.log(4.0) - 2.0794415 * jax.random.uniform(key_list[14], (PE, RE), jnp.float32) ** block_scale(key_list[14], (PE, RE), ((0, 8),), -0.2, 0.2)), 0.5, 4.0)
    intersect_env = normal_values(key_list[15], (PE, NB, RE, RE), (RE // 2) ** -0.5, 1.25, ((0, 8),))
    fock_env = jnp.clip(jax.random.uniform(key_list[16], (PE, NB), jnp.float32, -2.0, 2.0) * block_scale(key_list[16], (PE, NB), ((0, 8),), -0.4, 0.0), -2.0, 2.0)
    neighbor_env = set_ends(jax.random.randint(key_list[17], (PE, NB), 0, PE), jax.random.fold_in(key_list[17], 1), 0, PE - 1).astype(jnp.int32)
    return dict(left_active=left_active, right_active=right_active, amps_active=amps_active, rank_active=rank_active, gap_active=gap_active, energy_active=energy_active, intersect_active=intersect_active, fock_active=fock_active, neighbor_active=neighbor_active, left_env=left_env, right_env=right_env, amps_env=amps_env, rank_env=rank_env, gap_env=gap_env, energy_env=energy_env, intersect_env=intersect_env, fock_env=fock_env, neighbor_env=neighbor_env)


HIGHEST = lax.Precision.HIGHEST


def rank_masks(pair_ranks, full_width):
    positions = jnp.arange(full_width, dtype=jnp.int32)
    return (positions[None, :, None] < pair_ranks[:, None, None]) & (positions[None, None, :] < pair_ranks[:, None, None])


def update_level(left_ints, right_ints, amplitudes, pair_ranks, pair_gaps, energy, intersect, fock_weights, neighbor, with_ladder):
    full_width = amplitudes.shape[1]
    inside = rank_masks(pair_ranks, full_width)
    masked = jnp.where(inside, amplitudes, jnp.zeros_like(amplitudes))

    def one_pair(pair_items):
        left_pair, right_pair, amp_pair, over_pair, fock_pair, neigh_pair = pair_items
        summed_terms = jnp.dot(left_pair, right_pair.T, preferred_element_type=jnp.float32)
        if with_ladder:
            cross_left = jnp.dot(amp_pair.T, left_pair, preferred_element_type=jnp.float32).astype(jnp.bfloat16)
            cross_right = jnp.dot(amp_pair, right_pair, preferred_element_type=jnp.float32).astype(jnp.bfloat16)
            summed_terms = summed_terms + jnp.dot(cross_left, right_pair.T, preferred_element_type=jnp.float32)
            summed_terms = summed_terms + jnp.dot(cross_left, cross_right.T, preferred_element_type=jnp.float32)
        near_amps = masked[neigh_pair]
        half_product = jnp.einsum('krs,kst->krt', over_pair, near_amps, preferred_element_type=jnp.float32)
        full_product = jnp.einsum('krt,kut->kru', half_product, over_pair.astype(jnp.float32), precision=HIGHEST)
        return summed_terms + jnp.einsum('k,kru->ru', fock_pair, full_product, precision=HIGHEST)

    residual = lax.map(one_pair, (left_ints, right_ints, masked, intersect, fock_weights, neighbor))
    denominator = energy[:, :, None] + energy[:, None, :] + pair_gaps[:, None, None]
    return jnp.where(inside, masked.astype(jnp.float32) - residual / denominator, jnp.float32(0.0))


def reference(left_active, right_active, amps_active, rank_active, gap_active, energy_active, intersect_active, fock_active, neighbor_active, left_env, right_env, amps_env, rank_env, gap_env, energy_env, intersect_env, fock_env, neighbor_env):
    new_active = update_level(left_active, right_active, amps_active, rank_active, gap_active, energy_active, intersect_active, fock_active, neighbor_active, True)
    new_env = update_level(left_env, right_env, amps_env, rank_env, gap_env, energy_env, intersect_env, fock_env, neighbor_env, False)
    return (new_active, new_env)
```

```python
import jax
import jax.numpy as jnp
from jax import lax
from jax.experimental import pallas as pl
from jax.experimental.pallas import tpu as pltpu
from jax.sharding import PartitionSpec as P

BF16 = jnp.bfloat16
F32 = jnp.float32
VMEM = pl.BlockSpec(memory_space=pltpu.VMEM)
SMEM = pl.BlockSpec(memory_space=pltpu.SMEM)
HBM = pl.BlockSpec(memory_space=pl.ANY)


def dot_nt(left, right):
    return lax.dot_general(left, right, (((1,), (1,)), ((), ())), preferred_element_type=F32)


def dot_nn(left, right):
    return lax.dot_general(left, right, (((1,), (0,)), ((), ())), preferred_element_type=F32)


def dot_tn(left, right):
    return lax.dot_general(left, right, (((0,), (0,)), ((), ())), preferred_element_type=F32)


def cost(flops, nbytes):
    return pl.CostEstimate(flops=flops, bytes_accessed=nbytes, transcendentals=0)


def masked_rows(amps, rank, start):
    rows = start + lax.broadcasted_iota(jnp.int32, amps.shape, 0)
    cols = lax.broadcasted_iota(jnp.int32, amps.shape, 1)
    return jnp.where((rows < rank) & (cols < rank), amps, 0.0)


def pack_kernel(act_ref, env_ref, rank_ref, rank_env_ref, aux_ref, pair_ref):
    place = lax.axis_index("aux")
    n_act, rows_act, _ = act_ref.shape
    n_env, rows_env, width_env = env_ref.shape
    for p in range(n_act):
        block = masked_rows(act_ref[p].astype(F32), rank_ref[p], place * rows_act).astype(BF16)
        for dest in range(aux_ref.shape[0]):
            aux_ref[dest, p] = block
        for dest in range(pair_ref.shape[0]):
            pair_ref[dest, p] = block
    pair_ref[:, n_act:] = jnp.zeros((pair_ref.shape[0], n_env, 8, 128), BF16)
    for p in range(n_env):
        block = masked_rows(env_ref[p].astype(F32), rank_env_ref[p], place * rows_env).astype(BF16)
        for dest in range(pair_ref.shape[0]):
            pair_ref[dest, n_act + p, 0:rows_env, 0:width_env] = block


def ladder_kernel(la_ref, ra_ref, le_ref, re_ref, sa_ref, se_ref, la, ra, le, re, sems):
    n_act, n_env = la_ref.shape[0], le_ref.shape[0]
    copies = []
    for p in range(n_act):
        copies.append((
            pltpu.make_async_copy(la_ref.at[p], la.at[p], sems.at[0, p]),
            pltpu.make_async_copy(ra_ref.at[p], ra.at[p], sems.at[1, p]),
        ))
    for p in range(n_env):
        copies.append((
            pltpu.make_async_copy(le_ref.at[p], le.at[p], sems.at[0, n_act + p]),
            pltpu.make_async_copy(re_ref.at[p], re.at[p], sems.at[1, n_act + p]),
        ))
    for first, second in copies:
        first.start()
        second.start()
    for p in range(n_act):
        copies[p][0].wait()
        copies[p][1].wait()
        sa_ref[p] = dot_nt(la[p], ra[p])
    for p in range(n_env):
        copies[n_act + p][0].wait()
        copies[n_act + p][1].wait()
        se_ref[p] = dot_nt(le[p], re[p])


def combine_kernel(
    sa_ref, se_ref, own_ref, near_ref, xa_ref, xe_ref, fa_ref, na_ref, fe_ref, ne_ref, out_ref
):
    place = lax.axis_index("aux")
    n_act, n_env = sa_ref.shape[0], se_ref.shape[0]
    n_aux = own_ref.shape[0]
    width, width_env = sa_ref.shape[1], se_ref.shape[1]
    rows_env = width_env // n_aux
    tile = lax.broadcasted_iota(jnp.int32, (n_aux, 8, width), 0)
    for p in range(n_act):
        amps = own_ref[:, p].reshape(width, width)
        base = sa_ref[p]
        once = dot_tn(amps, base.astype(BF16))
        twice = dot_nt(once.astype(BF16), amps)
        halves = []
        for k in range(4):
            n = na_ref[p, k]
            near = near_ref[n // n_act, n % n_act]
            half = dot_nt(near, xa_ref[p, k]) * fa_ref[p, k]
            half = jnp.where(tile == place, half[None], 0.0).reshape(width, width)
            halves.append(half.astype(BF16))
        coupled = dot_nn(
            jnp.concatenate([xa_ref[p, k] for k in range(4)], axis=1),
            jnp.concatenate(halves, axis=0),
        )
        total = base + once + twice + coupled
        out_ref[:, p] = total.astype(BF16).reshape(n_aux, 8, width)
    row = lax.broadcasted_iota(jnp.int32, (width_env, 8), 0)
    col = lax.broadcasted_iota(jnp.int32, (width_env, 8), 1)
    pick = jnp.where((row == place * rows_env + col) & (col < rows_env), 1.0, 0.0).astype(BF16)
    env = []
    for p in range(n_env):
        total = se_ref[p]
        for k in range(4):
            n = ne_ref[p, k]
            near = near_ref[n // n_env, n_act + n % n_env][:, 0:width_env]
            half = dot_nt(near, xe_ref[p, k]) * fe_ref[p, k]
            cols = dot_nn(xe_ref[p, k], pick)
            total = total + dot_nn(cols.astype(BF16), half.astype(BF16))
        env.append(total.astype(BF16))
    row = lax.broadcasted_iota(jnp.int32, (n_aux * 8, 2 * width_env), 0)
    col = lax.broadcasted_iota(jnp.int32, (n_aux * 8, 2 * width_env), 1)
    slot = row % 8
    source = jnp.where(slot < rows_env, slot, width_env + slot - rows_env) + rows_env * (row // 8)
    spread = jnp.where((col == source) & (slot < 2 * rows_env), 1.0, 0.0).astype(BF16)
    out_ref[:, n_act] = jnp.zeros((n_aux, 8, width), BF16)
    for side in range(2):
        both = jnp.concatenate([env[2 * side], env[2 * side + 1]], axis=0)
        laid = dot_nn(spread, both).astype(BF16).reshape(n_aux, 8, width_env)
        out_ref[:, n_act, :, 64 * side : 64 * side + width_env] = laid


def own_energies(energy, shape, start):
    row = lax.broadcasted_iota(jnp.int32, shape, 0)
    col = lax.broadcasted_iota(jnp.int32, shape, 1)
    return jnp.sum(jnp.where(col == start + row, energy, 0.0), axis=1, keepdims=True)


def updated(amps, summed, energy, rank, gap, start):
    denominator = own_energies(energy, amps.shape, start) + energy + gap
    rows = start + lax.broadcasted_iota(jnp.int32, amps.shape, 0)
    cols = lax.broadcasted_iota(jnp.int32, amps.shape, 1)
    return jnp.where((rows < rank) & (cols < rank), amps - summed / denominator, 0.0)


def finish_kernel(
    sum_ref, aa_ref, ra_ref, ga_ref, ea_ref, ae_ref, re_ref, ge_ref, ee_ref, oa_ref, oe_ref
):
    place = lax.axis_index("aux")
    n_act, rows_act, _ = aa_ref.shape
    n_env, rows_env, width_env = ae_ref.shape
    for p in range(n_act):
        summed = jnp.sum(sum_ref[:, p].astype(F32), axis=0)
        oa_ref[p] = updated(
            aa_ref[p].astype(F32), summed, ea_ref[p : p + 1], ra_ref[p], ga_ref[p], place * rows_act
        )
    summed = jnp.sum(sum_ref[:, n_act].astype(F32), axis=0)
    for p in range(n_env):
        side, at = p // 2, rows_env * (p % 2)
        mine = summed[at : at + rows_env, 64 * side : 64 * side + width_env]
        oe_ref[p] = updated(
            ae_ref[p].astype(F32), mine, ee_ref[p : p + 1], re_ref[p], ge_ref[p], place * rows_env
        )


def shards(
    left_active, right_active, amps_active, rank_active, gap_active, energy_active,
    intersect_active, fock_active, neighbor_active,
    left_env, right_env, amps_env, rank_env, gap_env, energy_env,
    intersect_env, fock_env, neighbor_env,
):
    n_act, rows_act, width = amps_active.shape
    n_env, rows_env, width_env = amps_env.shape
    n_aux, n_pair = lax.axis_size("aux"), lax.axis_size("pair")
    shape = jax.ShapeDtypeStruct
    for_aux, for_pair = pl.pallas_call(
        pack_kernel,
        out_shape=(
            shape((n_aux, n_act, 8, 128), BF16),
            shape((n_pair, n_act + n_env, 8, 128), BF16),
        ),
        in_specs=[VMEM, VMEM, SMEM, SMEM],
        out_specs=(VMEM, VMEM),
        cost_estimate=cost(10**6, 10**6),
        name="pack",
    )(amps_active, amps_env, rank_active, rank_env)
    own = lax.all_to_all(for_aux, "aux", 0, 0, tiled=True)
    near = lax.all_to_all(for_pair, "pair", 0, 0, tiled=True)
    length = left_active.shape[2]
    sum_act, sum_env = pl.pallas_call(
        ladder_kernel,
        out_shape=(
            shape((n_act, width, width), F32),
            shape((n_env, width_env, width_env), F32),
        ),
        in_specs=[HBM] * 4,
        out_specs=(VMEM, VMEM),
        scratch_shapes=[
            pltpu.VMEM((n_act, width, length), BF16),
            pltpu.VMEM((n_act, width, length), BF16),
            pltpu.VMEM((n_env, width_env, length), BF16),
            pltpu.VMEM((n_env, width_env, length), BF16),
            pltpu.SemaphoreType.DMA((2, n_act + n_env)),
        ],
        compiler_params=pltpu.CompilerParams(vmem_limit_bytes=36 * 1024 * 1024),
        cost_estimate=cost(3 * 10**9, 23 * 10**6),
        name="ladder",
    )(left_active, right_active, left_env, right_env)
    shares = pl.pallas_call(
        combine_kernel,
        out_shape=shape((n_aux, n_act + 1, 8, 128), BF16),
        in_specs=[VMEM] * 6 + [SMEM] * 4,
        out_specs=VMEM,
        cost_estimate=cost(10**9, 3 * 10**6),
        name="combine",
    )(
        sum_act, sum_env, own, near, intersect_active, intersect_env,
        fock_active, neighbor_active, fock_env, neighbor_env,
    )
    summed = lax.all_to_all(shares, "aux", 0, 0, tiled=True)
    return pl.pallas_call(
        finish_kernel,
        out_shape=(
            shape((n_act, rows_act, width), F32),
            shape((n_env, rows_env, width_env), F32),
        ),
        in_specs=[VMEM, VMEM, SMEM, SMEM, VMEM, VMEM, SMEM, SMEM, VMEM],
        out_specs=(VMEM, VMEM),
        cost_estimate=cost(10**6, 10**6),
        name="finish",
    )(
        summed, amps_active, rank_active, gap_active, energy_active,
        amps_env, rank_env, gap_env, energy_env,
    )


def solution(mesh):
    rows = P("pair", "aux", None)
    deep = P("pair", None, "aux")
    per_pair = P("pair")
    level = (
        deep, deep, rows, per_pair, per_pair, P("pair", None),
        P("pair", None, None, None), P("pair", None), P("pair", None),
    )
    return jax.shard_map(
        shards, mesh=mesh, in_specs=level + level, out_specs=(rows, rows), check_vma=False
    )
```

```python
import jax
import jax.numpy as jnp
from jax import lax
from jax.experimental import pallas as pl
from jax.experimental.pallas import tpu as pltpu
from jax.sharding import PartitionSpec as P


BF16 = jnp.bfloat16
F32 = jnp.float32
VMEM = pl.BlockSpec(memory_space=pltpu.VMEM)
SMEM = pl.BlockSpec(memory_space=pltpu.SMEM)
HBM = pl.BlockSpec(memory_space=pl.ANY)
BIG = pltpu.CompilerParams(vmem_limit_bytes=60 * 1024 * 1024)
SMALL = pltpu.CompilerParams(vmem_limit_bytes=8 * 1024 * 1024)


def dot_nt(left, right):
    return lax.dot_general(left, right, (((1,), (1,)), ((), ())), preferred_element_type=F32)


def dot_nn(left, right):
    return lax.dot_general(left, right, (((1,), (0,)), ((), ())), preferred_element_type=F32)


def dot_tn(left, right):
    return lax.dot_general(left, right, (((0,), (0,)), ((), ())), preferred_element_type=F32)


def cost(flops, nbytes):
    return pl.CostEstimate(flops=flops, bytes_accessed=nbytes, transcendentals=0)


def masked_rows(amps, rank, start):
    rows = start + lax.broadcasted_iota(jnp.int32, amps.shape, 0)
    cols = lax.broadcasted_iota(jnp.int32, amps.shape, 1)
    return jnp.where((rows < rank) & (cols < rank), amps, 0.0)


def pack_kernel(act_ref, env_ref, rank_ref, rank_env_ref, aux_ref, block_ref):
    place = lax.axis_index("aux")
    n_act, rows_act, _ = act_ref.shape
    rows_env, n_env, width_env = env_ref.shape
    for p in range(n_act):
        block = masked_rows(act_ref[p].astype(F32), rank_ref[p], place * rows_act).astype(BF16)
        for dest in range(aux_ref.shape[0]):
            aux_ref[dest, p] = block
        block_ref[p] = block
    block_ref[n_act:] = jnp.zeros((n_env, 8, 128), BF16)
    for p in range(n_env):
        block = masked_rows(env_ref[:, p].astype(F32), rank_env_ref[p], place * rows_env).astype(BF16)
        block_ref[n_act + p, 0:rows_env, 0:width_env] = block


def mark_kernel(block_ref, mark_ref):
    mark_ref[...] = jnp.zeros(mark_ref.shape, F32)


def ladder_kernel(la_ref, ra_ref, le_ref, re_ref, own_ref, mark_ref, sa_ref, se_ref):
    width = sa_ref.shape[1]
    for p in range(la_ref.shape[0]):
        sa_ref[p] = dot_nt(la_ref[p], ra_ref[p])
    for p in range(la_ref.shape[0]):
        amps = own_ref[:, p].reshape(width, width)
        base = sa_ref[p]
        once = dot_tn(amps, base.astype(BF16))
        twice = dot_nt(once.astype(BF16), amps)
        sa_ref[p] = base + once + twice
    for p in range(le_ref.shape[0]):
        se_ref[p] = dot_nt(le_ref[p], re_ref[p])


def combine_kernel(sa_ref, se_ref, *refs):
    n_near = len(refs) - 8
    near_refs = refs[:n_near]
    xa_ref, xe_ref, fa_ref, na_ref, fe_ref, ne_ref, out_ref, near_ref = refs[n_near:]
    place, group = lax.axis_index("aux"), lax.axis_index("pair")
    n_aux, (n_act, width, _) = out_ref.shape[0], sa_ref.shape
    n_env, width_env, _ = se_ref.shape
    rows_env = width_env // n_aux
    tile = lax.broadcasted_iota(jnp.int32, (n_aux, 8, width), 0)
    chips = n_near // 2
    for slot in range(n_near):
        near_ref[slot] = near_refs[slot][...]

    def near_block(n, count, first):
        source = n // count
        slot = (group // 2 + chips - source // 2) % chips + chips * ((group + source) % 2)
        return near_ref[slot, first + n % count]

    for p in range(n_act):
        halves = []
        for k in range(4):
            half = dot_nt(near_block(na_ref[k, p], n_act, 0), xa_ref[p, k]) * fa_ref[k, p]
            half = jnp.where(tile == place, half[None], 0.0).reshape(width, width)
            halves.append(half.astype(BF16))
        coupled = dot_nn(
            jnp.concatenate([xa_ref[p, k] for k in range(4)], axis=1),
            jnp.concatenate(halves, axis=0),
        )
        out_ref[:, p] = (sa_ref[p] + coupled).astype(BF16).reshape(n_aux, 8, width)
    row = lax.broadcasted_iota(jnp.int32, (width_env, 8), 0)
    col = lax.broadcasted_iota(jnp.int32, (width_env, 8), 1)
    pick = jnp.where((row == place * rows_env + col) & (col < rows_env), 1.0, 0.0).astype(BF16)
    env = []
    for p in range(n_env):
        total = se_ref[p]
        for k in range(4):
            near = near_block(ne_ref[p, k], n_env, n_act)[:, 0:width_env]
            half = dot_nt(near, xe_ref[p, k]) * fe_ref[p, k]
            cols = dot_nn(xe_ref[p, k], pick)
            total = total + dot_nn(cols.astype(BF16), half.astype(BF16))
        env.append(total.astype(BF16))
    row = lax.broadcasted_iota(jnp.int32, (n_aux * 8, 2 * width_env), 0)
    col = lax.broadcasted_iota(jnp.int32, (n_aux * 8, 2 * width_env), 1)
    slot = row % 8
    source = jnp.where(slot < rows_env, slot, width_env + slot - rows_env) + rows_env * (row // 8)
    spread = jnp.where((col == source) & (slot < 2 * rows_env), 1.0, 0.0).astype(BF16)
    out_ref[:, n_act] = jnp.zeros((n_aux, 8, width), BF16)
    for side in range(2):
        both = jnp.concatenate([env[2 * side], env[2 * side + 1]], axis=0)
        laid = dot_nn(spread, both).astype(BF16).reshape(n_aux, 8, width_env)
        out_ref[:, n_act, :, 64 * side : 64 * side + width_env] = laid


def own_energies(energy, shape, start):
    row = lax.broadcasted_iota(jnp.int32, shape, 0)
    col = lax.broadcasted_iota(jnp.int32, shape, 1)
    return jnp.sum(jnp.where(col == start + row, energy, 0.0), axis=1, keepdims=True)


def updated(amps, summed, energy, rank, gap, start):
    denominator = own_energies(energy, amps.shape, start) + energy + gap
    rows = start + lax.broadcasted_iota(jnp.int32, amps.shape, 0)
    cols = lax.broadcasted_iota(jnp.int32, amps.shape, 1)
    return jnp.where((rows < rank) & (cols < rank), amps - summed / denominator, 0.0)


def finish_kernel(
    sum_ref, aa_ref, ra_ref, ga_ref, ea_ref, ae_ref, re_ref, ge_ref, ee_ref, oa_ref, oe_ref
):
    place = lax.axis_index("aux")
    n_act, rows_act, _ = aa_ref.shape
    rows_env, n_env, width_env = ae_ref.shape
    for p in range(n_act):
        summed = jnp.sum(sum_ref[:, p].astype(F32), axis=0)
        oa_ref[p] = updated(
            aa_ref[p].astype(F32), summed, ea_ref[p : p + 1], ra_ref[p], ga_ref[p], place * rows_act
        )
    summed = jnp.sum(sum_ref[:, n_act].astype(F32), axis=0)
    for p in range(n_env):
        side, at = p // 2, rows_env * (p % 2)
        mine = summed[at : at + rows_env, 64 * side : 64 * side + width_env]
        oe_ref[:, p] = updated(
            ae_ref[:, p].astype(F32), mine, ee_ref[p : p + 1], re_ref[p], ge_ref[p], place * rows_env
        )


def shards(
    left_active, right_active, amps_active, rank_active, gap_active, energy_active,
    intersect_active, fock_active, neighbor_active,
    left_env, right_env, amps_env, rank_env, gap_env, energy_env,
    intersect_env, fock_env, neighbor_env,
):
    n_act, rows_act, width = amps_active.shape
    n_env, rows_env, width_env = amps_env.shape
    n_aux, n_pair = lax.axis_size("aux"), lax.axis_size("pair")
    shape = jax.ShapeDtypeStruct
    amps_env_t = amps_env.transpose(1, 0, 2)
    for_aux, block = pl.pallas_call(
        pack_kernel,
        out_shape=(
            shape((n_aux, n_act, 8, 128), BF16),
            shape((n_act + n_env, 8, 128), BF16),
        ),
        in_specs=[VMEM, VMEM, SMEM, SMEM],
        out_specs=(VMEM, VMEM),
        compiler_params=BIG,
        cost_estimate=cost(10**6, 10**6),
        name="pack",
    )(amps_active, amps_env_t, rank_active, rank_env)
    ring, near = [block], []
    mark = pl.pallas_call(
        mark_kernel,
        out_shape=shape((8, 128), F32),
        in_specs=[HBM],
        out_specs=VMEM,
        compiler_params=SMALL,
        cost_estimate=cost(3 * 10**10, 10**4),
        name="mark",
    )(block)
    for step in range(1, n_pair // 2):
        route = [(i, (i + 2 * step) % n_pair) for i in range(n_pair)]
        ring.append(lax.ppermute(block, "pair", route))
    own = lax.all_to_all(for_aux, "aux", 0, 0, tiled=True)
    partner = [(i, i ^ 1) for i in range(n_pair)]
    near = ring + [lax.ppermute(x, "pair", partner) for x in ring]
    sum_act, sum_env = pl.pallas_call(
        ladder_kernel,
        out_shape=[shape((n_act, width, width), F32), shape((n_env, width_env, width_env), F32)],
        in_specs=[VMEM] * 5 + [HBM],
        out_specs=[VMEM] * 2,
        compiler_params=SMALL,
        cost_estimate=cost(3 * 10**9, 23 * 10**6),
        name="ladder",
    )(left_active, right_active, left_env, right_env, own, mark)
    shares = pl.pallas_call(
        combine_kernel,
        out_shape=shape((n_aux, n_act + 1, 8, 128), BF16),
        in_specs=[VMEM] * (4 + len(near)) + [SMEM] * 4,
        out_specs=VMEM,
        scratch_shapes=[
            pltpu.VMEM((len(near), n_act + n_env, 8, 128), BF16),
        ],
        compiler_params=SMALL,
        cost_estimate=cost(10**9, 3 * 10**6),
        name="combine",
    )(
        sum_act, sum_env, *near, intersect_active, intersect_env,
        fock_active.T, neighbor_active.T, fock_env, neighbor_env,
    )
    summed = lax.all_to_all(shares, "aux", 0, 0, tiled=True)
    new_active, new_env = pl.pallas_call(
        finish_kernel,
        out_shape=(
            shape((n_act, rows_act, width), F32),
            shape((rows_env, n_env, width_env), F32),
        ),
        in_specs=[VMEM, VMEM, SMEM, SMEM, VMEM, VMEM, SMEM, SMEM, VMEM],
        out_specs=(VMEM, VMEM),
        compiler_params=SMALL,
        cost_estimate=cost(10**6, 10**6),
        name="finish",
    )(
        summed, amps_active, rank_active, gap_active, energy_active,
        amps_env_t, rank_env, gap_env, energy_env,
    )
    return new_active, new_env.transpose(1, 0, 2)


def solution(mesh):
    rows = P("pair", "aux", None)
    deep = P("pair", None, "aux")
    per_pair = P("pair")
    level = (
        deep, deep, rows, per_pair, per_pair, P("pair", None),
        P("pair", None, None, None), P("pair", None), P("pair", None),
    )
    return jax.shard_map(
        shards, mesh=mesh, in_specs=level + level, out_specs=(rows, rows), check_vma=False
    )
```

```python
import jax
import jax.numpy as jnp
from jax import lax
from jax.experimental import pallas as pl
from jax.experimental.pallas import tpu as pltpu
from jax.sharding import PartitionSpec as P


BF16 = jnp.bfloat16
F32 = jnp.float32
VMEM = pl.BlockSpec(memory_space=pltpu.VMEM)
SMEM = pl.BlockSpec(memory_space=pltpu.SMEM)
HBM = pl.BlockSpec(memory_space=pl.ANY)
MARK = 3 * 10**10
BIG = pltpu.CompilerParams(vmem_limit_bytes=60 * 1024 * 1024)
SMALL = pltpu.CompilerParams(vmem_limit_bytes=8 * 1024 * 1024)


def dot(left, right, contract):
    return lax.dot_general(left, right, ((contract[:1], contract[1:]), ((), ())), preferred_element_type=F32)


def dot_nt(left, right):
    return dot(left, right, (1, 1))


def dot_nn(left, right):
    return dot(left, right, (1, 0))


def dot_tn(left, right):
    return dot(left, right, (0, 0))


def own_energies(energy, shape, start):
    row = lax.broadcasted_iota(jnp.int32, shape, 0)
    col = lax.broadcasted_iota(jnp.int32, shape, 1)
    return jnp.sum(jnp.where(col == start + row, energy, 0.0), axis=1, keepdims=True)


def inside(shape, rank, start):
    rows = start + lax.broadcasted_iota(jnp.int32, shape, 0)
    return (rows < rank) & (lax.broadcasted_iota(jnp.int32, shape, 1) < rank)


def pack_kernel(
    aa_ref, ra_ref, ga_ref, ea_ref, ae_ref, re_ref, ge_ref, ee_ref, block_ref, scale_a_ref, scale_e_ref
):
    place = lax.axis_index("aux")
    n_act, rows_act, _ = aa_ref.shape
    rows_env, n_env, width_env = ae_ref.shape

    def prepare(amps, rank, gap, energy, start):
        keep = inside(amps.shape, rank, start)
        scale = 1.0 / (own_energies(energy, amps.shape, start) + energy + gap)
        return jnp.where(keep, amps.astype(F32), 0.0).astype(BF16), jnp.where(keep, scale, 0.0)

    for p in range(n_act):
        block_ref[p], scale_a_ref[p] = prepare(
            aa_ref[p], ra_ref[p], ga_ref[p], ea_ref[p : p + 1], place * rows_act
        )
    block_ref[n_act:] = jnp.zeros((n_env, 8, 128), BF16)
    for p in range(n_env):
        block_ref[n_act + p, 0:rows_env, 0:width_env], scale_e_ref[:, p] = prepare(
            ae_ref[:, p], re_ref[p], ge_ref[p], ee_ref[p : p + 1], place * rows_env
        )


def mark_kernel(_, mark_ref):
    mark_ref[...] = jnp.zeros(mark_ref.shape, F32)


def stack_kernel(*refs):
    for i, ref in enumerate(refs[:-1]):
        refs[-1][i] = ref[0 : refs[-1].shape[1]]


def main_kernel(la_ref, ra_ref, le_ref, re_ref, mark_ref, *refs):
    n_near = len(refs) - 15
    near_refs = refs[:n_near]
    xa_ref, xe_ref, *tables, sa_ref, ca_ref, se_ref, near_ref = refs[n_near : n_near + 10]
    fa_ref, na_ref, fe_ref, ne_ref, sems = refs[n_near + 10 :]
    copies = [
        pltpu.make_async_copy(source, target, sems.at[i])
        for i, (source, target) in enumerate(zip(tables, (fa_ref, na_ref, fe_ref, ne_ref)))
    ]
    for copy in copies:
        copy.start()
    place, group = lax.axis_index("aux"), lax.axis_index("pair")
    n_act, width, _ = sa_ref.shape
    n_env, width_env, _ = se_ref.shape
    rows_env = width_env // (width // 8)
    for slot in range(n_near):
        near_ref[slot] = near_refs[slot][...]
    for p in range(n_act):
        sa_ref[p] = dot_nt(la_ref[p], ra_ref[p])
    for p in range(n_env):
        se_ref[p] = dot_nt(le_ref[p], re_ref[p])
    for copy in copies:
        copy.wait()

    def near_block(n, count, first):
        source = n // count
        slot = (group // 2 + n_near - source // 2) % n_near
        return near_ref[slot, (group + source) % 2, first + n % count]

    lane = lax.broadcasted_iota(jnp.int32, (width, width), 1) // 8
    for p in range(n_act):
        halves, cols = [], jnp.zeros((width, width), F32)
        for k in range(4):
            near = near_block(na_ref[k, p], n_act, 0)
            halves.append(dot_nt(near, xa_ref[p, k]) * fa_ref[k, p])
            turned = pltpu.roll(xa_ref[p, k].astype(F32), (width + 8 * k - 8 * place) % width, 1)
            cols = jnp.where(lane == k, turned, cols)
        halves.append(jnp.zeros((width - 32, width), F32))
        ca_ref[p] = dot_nn(cols.astype(BF16), jnp.concatenate(halves, axis=0).astype(BF16))
    row = lax.broadcasted_iota(jnp.int32, (width_env, 8), 0)
    col = lax.broadcasted_iota(jnp.int32, (width_env, 8), 1)
    pick = jnp.where((row == place * rows_env + col) & (col < rows_env), 1.0, 0.0).astype(BF16)
    for p in range(n_env):
        total = se_ref[p]
        for k in range(4):
            near = near_block(ne_ref[p, k], n_env, n_act)[:, 0:width_env]
            half = dot_nt(near, xe_ref[p, k]) * fe_ref[p, k]
            cols = dot_nn(xe_ref[p, k], pick)
            total = total + dot_nn(cols.astype(BF16), half.astype(BF16))
        se_ref[p] = total


def combine_kernel(sa_ref, ca_ref, se_ref, *refs):
    own_refs, (out_ref, own_ref) = refs[:-2], refs[-2:]
    place = lax.axis_index("aux")
    n_own = len(own_refs)
    n_aux, (n_act, width, _) = out_ref.shape[0], sa_ref.shape
    n_env, width_env, _ = se_ref.shape
    rows_env = width_env // n_aux
    side = own_refs[0].shape[0]
    for dz in range(n_own):
        for dy in range(side):
            y = (place // n_own + side - dy) % side
            own_ref[y * n_own + (place + n_own - dz) % n_own] = own_refs[dz][dy]
    for p in range(n_act):
        amps = own_ref[:, p].reshape(width, width)
        base = sa_ref[p]
        once = dot_tn(amps, base.astype(BF16))
        twice = dot_nt(once.astype(BF16), amps)
        total = base + once + twice + ca_ref[p]
        out_ref[:, p] = total.astype(BF16).reshape(n_aux, 8, width)
    env = [se_ref[p].astype(BF16) for p in range(n_env)]
    row = lax.broadcasted_iota(jnp.int32, (n_aux * 8, 2 * width_env), 0)
    col = lax.broadcasted_iota(jnp.int32, (n_aux * 8, 2 * width_env), 1)
    slot = row % 8
    source = jnp.where(slot < rows_env, slot, width_env + slot - rows_env) + rows_env * (row // 8)
    spread = jnp.where((col == source) & (slot < 2 * rows_env), 1.0, 0.0).astype(BF16)
    out_ref[:, n_act] = jnp.zeros((n_aux, 8, width), BF16)
    for half in range(2):
        both = jnp.concatenate([env[2 * half], env[2 * half + 1]], axis=0)
        laid = dot_nn(spread, both).astype(BF16).reshape(n_aux, 8, width_env)
        out_ref[:, n_act, :, 64 * half : 64 * half + width_env] = laid


def finish_kernel(sum_ref, block_ref, scale_a_ref, scale_e_ref, oa_ref, oe_ref):
    n_act = scale_a_ref.shape[0]
    rows_env, n_env, width_env = scale_e_ref.shape
    for p in range(n_act):
        summed = jnp.sum(sum_ref[:, p].astype(F32), axis=0)
        oa_ref[p] = block_ref[p].astype(F32) - summed * scale_a_ref[p]
    summed = jnp.sum(sum_ref[:, n_act].astype(F32), axis=0)
    for p in range(n_env):
        half, at = p // 2, rows_env * (p % 2)
        mine = summed[at : at + rows_env, 64 * half : 64 * half + width_env]
        amps = block_ref[n_act + p, 0:rows_env, 0:width_env].astype(F32)
        oe_ref[:, p] = amps - mine * scale_e_ref[:, p]


def shards(
    left_active, right_active, amps_active, rank_active, gap_active, energy_active,
    intersect_active, fock_active, neighbor_active,
    left_env, right_env, amps_env, rank_env, gap_env, energy_env,
    intersect_env, fock_env, neighbor_env,
):
    n_act, rows_act, width = amps_active.shape
    n_env, rows_env, width_env = amps_env.shape
    n_aux, n_pair, n_z = lax.axis_size("aux"), lax.axis_size("pair"), 4
    shape = jax.ShapeDtypeStruct

    def call(kernel, out, ins, *arrays, scratch=(), params=SMALL, flops=10**6):
        return pl.pallas_call(
            kernel,
            out_shape=out,
            in_specs=ins,
            out_specs=jax.tree.map(lambda _: VMEM, out),
            scratch_shapes=scratch,
            compiler_params=params,
            cost_estimate=pl.CostEstimate(flops=flops, bytes_accessed=10**6, transcendentals=0),
        )(*arrays)

    def moved(x, axis, size, route):
        return lax.ppermute(x, axis, [(i, route(i)) for i in range(size)])

    def stack(arrays, tiles):
        out = shape((len(arrays), tiles, 8, 128), BF16)
        return call(stack_kernel, out, [VMEM] * len(arrays), *arrays)

    block, scale_act, scale_env = call(
        pack_kernel,
        [
            shape((n_act + n_env, 8, 128), BF16),
            shape((n_act, rows_act, width), F32),
            shape((rows_env, n_env, width_env), F32),
        ],
        [VMEM, SMEM, SMEM, VMEM] * 2,
        amps_active, rank_active, gap_active, energy_active,
        amps_env.transpose(1, 0, 2), rank_env, gap_env, energy_env,
        params=BIG,
    )
    mark = call(mark_kernel, shape((8, 128), F32), [HBM], block, flops=MARK)
    other = moved(block, "pair", n_pair, lambda i: i ^ 1)
    own = [block]
    for step in range(1, n_aux // n_z):
        own.append(moved(block, "aux", n_aux, lambda i: (i + n_z * step) % n_aux))
    near = [stack([block, other], n_act + n_env)]
    for step in range(1, n_pair // 2):
        near.append(moved(near[0], "pair", n_pair, lambda i: (i + 2 * step) % n_pair))
    own = [stack(own, n_act)]
    for step in range(1, n_z):
        own.append(moved(own[0], "aux", n_aux, lambda i: i // n_z * n_z + (i + step) % n_z))
    sum_act, couple_act, sum_env = call(
        main_kernel,
        [shape((n_act, width, width), F32)] * 2 + [shape((n_env, width_env, width_env), F32)],
        [VMEM] * 4 + [HBM] + [VMEM] * (len(near) + 2) + [HBM] * 4,
        left_active, right_active, left_env, right_env, mark,
        *near, intersect_active, intersect_env, fock_active.T, neighbor_active.T, fock_env, neighbor_env,
        scratch=[
            pltpu.VMEM((len(near), 2, n_act + n_env, 8, 128), BF16),
            pltpu.SMEM((4, n_act), F32),
            pltpu.SMEM((4, n_act), jnp.int32),
            pltpu.SMEM((n_env, 4), F32),
            pltpu.SMEM((n_env, 4), jnp.int32),
            pltpu.SemaphoreType.DMA((4,)),
        ],
        flops=5 * 10**9,
    )
    shares = call(
        combine_kernel, shape((n_aux, n_act + 1, 8, 128), BF16), [VMEM] * (3 + len(own)),
        sum_act, couple_act, sum_env, *own,
        scratch=[pltpu.VMEM((n_aux, n_act, 8, 128), BF16)], flops=10**9,
    )
    summed = lax.all_to_all(shares, "aux", 0, 0, tiled=True)
    new_active, new_env = call(
        finish_kernel,
        [shape((n_act, rows_act, width), F32), shape((rows_env, n_env, width_env), F32)],
        [VMEM] * 4,
        summed, block, scale_act, scale_env,
    )
    return new_active, new_env.transpose(1, 0, 2)


def solution(mesh):
    rows = P("pair", "aux", None)
    deep = P("pair", None, "aux")
    per_pair = P("pair")
    level = (
        deep, deep, rows, per_pair, per_pair, P("pair", None),
        P("pair", None, None, None), P("pair", None), P("pair", None),
    )

    return jax.shard_map(
        shards, mesh=mesh, in_specs=level + level, out_specs=(rows, rows), check_vma=False
    )
```

```python
import jax
import jax.numpy as jnp
from jax import lax
from jax.experimental import pallas as pl
from jax.experimental.pallas import tpu as pltpu
from jax.sharding import PartitionSpec as P


BF16 = jnp.bfloat16
F32 = jnp.float32
VMEM = pl.BlockSpec(memory_space=pltpu.VMEM)
SMEM = pl.BlockSpec(memory_space=pltpu.SMEM)
HBM = pl.BlockSpec(memory_space=pl.ANY)
MARK = 3 * 10**10
BIG = pltpu.CompilerParams(vmem_limit_bytes=60 * 1024 * 1024)
SMALL = pltpu.CompilerParams(vmem_limit_bytes=8 * 1024 * 1024)


def dot(left, right, contract):
    return lax.dot_general(left, right, ((contract[:1], contract[1:]), ((), ())), preferred_element_type=F32)


def dot_nt(left, right):
    return dot(left, right, (1, 1))


def dot_nn(left, right):
    return dot(left, right, (1, 0))


def dot_tn(left, right):
    return dot(left, right, (0, 0))


def own_energies(energy, shape, start):
    row = lax.broadcasted_iota(jnp.int32, shape, 0)
    col = lax.broadcasted_iota(jnp.int32, shape, 1)
    return jnp.sum(jnp.where(col == start + row, energy, 0.0), axis=1, keepdims=True)


def inside(shape, rank, start):
    rows = start + lax.broadcasted_iota(jnp.int32, shape, 0)
    return (rows < rank) & (lax.broadcasted_iota(jnp.int32, shape, 1) < rank)


def pack_kernel(
    aa_ref, ra_ref, ga_ref, ea_ref, ae_ref, re_ref, ge_ref, ee_ref, block_ref, scale_a_ref, scale_e_ref
):
    place = lax.axis_index("aux")
    n_act, rows_act, _ = aa_ref.shape
    rows_env, n_env, width_env = ae_ref.shape

    def prepare(amps, rank, gap, energy, start):
        keep = inside(amps.shape, rank, start)
        scale = 1.0 / (own_energies(energy, amps.shape, start) + energy + gap)
        return jnp.where(keep, amps.astype(F32), 0.0).astype(BF16), jnp.where(keep, scale, 0.0)

    for p in range(n_act):
        block_ref[p], scale_a_ref[p] = prepare(
            aa_ref[p], ra_ref[p], ga_ref[p], ea_ref[p : p + 1], place * rows_act
        )
    block_ref[n_act:] = jnp.zeros((n_env, 8, 128), BF16)
    for p in range(n_env):
        block_ref[n_act + p, 0:rows_env, 0:width_env], scale_e_ref[:, p] = prepare(
            ae_ref[:, p], re_ref[p], ge_ref[p], ee_ref[p : p + 1], place * rows_env
        )


def mark_kernel(mark_ref):
    mark_ref[...] = jnp.zeros(mark_ref.shape, F32)


def stack_kernel(*refs):
    for i, ref in enumerate(refs[:-1]):
        refs[-1][i] = ref[0 : refs[-1].shape[1]]


def main_kernel(la_ref, ra_ref, le_ref, re_ref, mark_ref, *refs):
    n_near = len(refs) - 18
    near_refs = refs[:n_near]
    xa_ref, xe_ref, *tables, sa_ref, ca_ref, se_ref, near_act, near_env = refs[n_near : n_near + 11]
    fa_ref, na_ref, fe_ref, ne_ref, sems, cols_ref, half_ref = refs[n_near + 11 :]
    copies = [
        pltpu.make_async_copy(source, target, sems.at[i])
        for i, (source, target) in enumerate(zip(tables, (fa_ref, na_ref, fe_ref, ne_ref)))
    ]
    for copy in copies:
        copy.start()
    place, group = lax.axis_index("aux"), lax.axis_index("pair")
    n_act, width, _ = sa_ref.shape
    n_env, width_env, _ = se_ref.shape
    rows_env = width_env // (width // 8)
    for slot in range(n_near):
        for core in range(2):
            source = 2 * lax.rem(group // 2 + n_near - slot, n_near) + lax.rem(group + core, 2)
            near_act[pl.ds(source * n_act, n_act)] = near_refs[slot][core, 0:n_act]
            near_env[pl.ds(source * n_env, n_env)] = near_refs[slot][core, n_act:]
    lane = lax.broadcasted_iota(jnp.int32, (width, width), 1) // 8
    for p in range(n_act):
        sa_ref[p] = dot_nt(la_ref[p], ra_ref[p])
        cols = 0.0
        for k in range(4):
            turned = pltpu.roll(xa_ref[p, k].astype(F32), (width + 8 * k - 8 * place) % width, 1)
            cols = jnp.where(lane == k, turned, cols)
        cols_ref[p] = cols.astype(BF16)
    for p in range(n_env):
        se_ref[p] = dot_nt(le_ref[p], re_ref[p])
    for copy in copies:
        copy.wait()

    row = lax.broadcasted_iota(jnp.int32, (32, width), 0) // 8
    for p in range(n_act):
        near, fock = [], 0.0
        for k in range(4):
            block = near_act[na_ref[k, p]]
            near.append(jnp.where(row == k, jnp.concatenate([block.astype(F32)] * 4, axis=0), 0.0))
            fock = jnp.where(row == k, fa_ref[k, p], fock)
        half = dot_nt(
            jnp.concatenate(near, axis=1).astype(BF16),
            jnp.concatenate([xa_ref[p, k] for k in range(4)], axis=1),
        )
        half_ref[p] = (half * fock).astype(BF16)
    for p in range(n_act):
        ca_ref[p] = dot_nn(cols_ref[p, :, 0:32], half_ref[p])
    count = 4 * n_env
    lane = lax.broadcasted_iota(jnp.int32, (width_env, 8 * count), 1) // 8
    near = [near_env[ne_ref[i // 4, i % 4]][:, 0:width_env].astype(F32) for i in range(count)]
    slot = lax.broadcasted_iota(jnp.int32, (8 * count, width_env), 0) % 8
    col = lax.broadcasted_iota(jnp.int32, (8 * count, width_env), 1)
    pick = jnp.where((col == place * rows_env + slot) & (slot < rows_env), 1.0, 0.0).astype(BF16)
    over = xe_ref[...].reshape(count * width_env, width_env)
    half = dot_nt(over, jnp.concatenate(near, axis=0).astype(BF16))
    cols = dot_nt(over, pick)
    for p in range(n_env):
        mine, theirs = 0.0, 0.0
        for i in range(4 * p, 4 * p + 4):
            at = slice(i * width_env, (i + 1) * width_env)
            theirs = jnp.where(lane == i, half[at] * fe_ref[p, i % 4], theirs)
            mine = jnp.where(lane == i, cols[at], mine)
        se_ref[p] += dot_nt(mine.astype(BF16), theirs.astype(BF16))


def combine_kernel(sa_ref, ca_ref, se_ref, *refs):
    own_refs, (out_ref, own_ref, once_ref) = refs[:-3], refs[-3:]
    place = lax.axis_index("aux")
    n_own = len(own_refs)
    n_aux, (n_act, width, _) = out_ref.shape[0], sa_ref.shape
    n_env, width_env, _ = se_ref.shape
    rows_env = width_env // n_aux
    side = own_refs[0].shape[0]
    for dz in range(n_own):
        for dy in range(side):
            y = (place // n_own + side - dy) % side
            own_ref[y * n_own + (place + n_own - dz) % n_own] = own_refs[dz][dy]
    for p in range(n_act):
        amps = own_ref[:, p].reshape(width, width)
        once_ref[p] = dot_tn(amps, sa_ref[p].astype(BF16))
    for p in range(n_act):
        amps = own_ref[:, p].reshape(width, width)
        once = once_ref[p]
        total = sa_ref[p] + ca_ref[p] + once + dot_nt(once.astype(BF16), amps)
        out_ref[:, p] = total.astype(BF16).reshape(n_aux, 8, width)
    env = [se_ref[p].astype(BF16) for p in range(n_env)]
    row = lax.broadcasted_iota(jnp.int32, (n_aux * 8, 2 * width_env), 0)
    col = lax.broadcasted_iota(jnp.int32, (n_aux * 8, 2 * width_env), 1)
    slot = row % 8
    source = jnp.where(slot < rows_env, slot, width_env + slot - rows_env) + rows_env * (row // 8)
    spread = jnp.where((col == source) & (slot < 2 * rows_env), 1.0, 0.0).astype(BF16)
    out_ref[:, n_act] = jnp.zeros((n_aux, 8, width), BF16)
    for half in range(2):
        both = jnp.concatenate([env[2 * half], env[2 * half + 1]], axis=0)
        laid = dot_nn(spread, both).astype(BF16).reshape(n_aux, 8, width_env)
        out_ref[:, n_act, :, 64 * half : 64 * half + width_env] = laid


def finish_kernel(sum_ref, block_ref, scale_a_ref, scale_e_ref, oa_ref, oe_ref):
    n_act = scale_a_ref.shape[0]
    rows_env, n_env, width_env = scale_e_ref.shape
    for p in range(n_act):
        summed = jnp.sum(sum_ref[:, p].astype(F32), axis=0)
        oa_ref[p] = block_ref[p].astype(F32) - summed * scale_a_ref[p]
    summed = jnp.sum(sum_ref[:, n_act].astype(F32), axis=0)
    for p in range(n_env):
        half, at = p // 2, rows_env * (p % 2)
        mine = summed[at : at + rows_env, 64 * half : 64 * half + width_env]
        amps = block_ref[n_act + p, 0:rows_env, 0:width_env].astype(F32)
        oe_ref[:, p] = amps - mine * scale_e_ref[:, p]


def shards(
    left_active, right_active, amps_active, rank_active, gap_active, energy_active,
    intersect_active, fock_active, neighbor_active,
    left_env, right_env, amps_env, rank_env, gap_env, energy_env,
    intersect_env, fock_env, neighbor_env,
):
    n_act, rows_act, width = amps_active.shape
    n_env, rows_env, width_env = amps_env.shape
    n_aux, n_pair, n_z = lax.axis_size("aux"), lax.axis_size("pair"), 4
    shape = jax.ShapeDtypeStruct

    def call(kernel, out, ins, *arrays, scratch=(), params=SMALL, flops=10**6):
        return pl.pallas_call(
            kernel,
            out_shape=out,
            in_specs=ins,
            out_specs=jax.tree.map(lambda _: VMEM, out),
            scratch_shapes=scratch,
            compiler_params=params,
            cost_estimate=pl.CostEstimate(flops=flops, bytes_accessed=10**6, transcendentals=0),
        )(*arrays)

    def moved(x, axis, size, route):
        return lax.ppermute(x, axis, [(i, route(i)) for i in range(size)])

    def stack(arrays, tiles):
        out = shape((len(arrays), tiles, 8, 128), BF16)
        return call(stack_kernel, out, [VMEM] * len(arrays), *arrays)

    mark = call(mark_kernel, shape((8, 128), F32), [], flops=MARK)
    block, scale_act, scale_env = call(
        pack_kernel,
        [
            shape((n_act + n_env, 8, 128), BF16),
            shape((n_act, rows_act, width), F32),
            shape((rows_env, n_env, width_env), F32),
        ],
        [VMEM, SMEM, SMEM, VMEM] * 2,
        amps_active, rank_active, gap_active, energy_active,
        amps_env.transpose(1, 0, 2), rank_env, gap_env, energy_env,
    )
    other = moved(block, "pair", n_pair, lambda i: i ^ 1)
    own = [block]
    for step in range(1, n_aux // n_z):
        own.append(moved(block, "aux", n_aux, lambda i: (i + n_z * step) % n_aux))
    near = [stack([block, other], n_act + n_env)]
    for step in range(1, n_pair // 2):
        near.append(moved(near[0], "pair", n_pair, lambda i: (i + 2 * step) % n_pair))
    own = [stack(own, n_act)]
    for step in range(1, n_z):
        own.append(moved(own[0], "aux", n_aux, lambda i: i // n_z * n_z + (i + step) % n_z))
    sum_act, couple_act, sum_env = call(
        main_kernel,
        [shape((n_act, width, width), F32)] * 2 + [shape((n_env, width_env, width_env), F32)],
        [VMEM] * 4 + [HBM] + [VMEM] * (len(near) + 2) + [HBM] * 4,
        left_active, right_active, left_env, right_env, mark,
        *near, intersect_active, intersect_env, fock_active.T, neighbor_active.T, fock_env, neighbor_env,
        scratch=[
            pltpu.VMEM((n_pair * n_act, 8, 128), BF16),
            pltpu.VMEM((n_pair * n_env, 8, 128), BF16),
            pltpu.SMEM((4, n_act), F32),
            pltpu.SMEM((4, n_act), jnp.int32),
            pltpu.SMEM((n_env, 4), F32),
            pltpu.SMEM((n_env, 4), jnp.int32),
            pltpu.SemaphoreType.DMA((4,)),
            pltpu.VMEM((n_act, width, width), BF16),
            pltpu.VMEM((n_act, 32, width), BF16),
        ],
        flops=5 * 10**9,
    )
    shares = call(
        combine_kernel, shape((n_aux, n_act + 1, 8, 128), BF16), [VMEM] * (3 + len(own)),
        sum_act, couple_act, sum_env, *own,
        scratch=[pltpu.VMEM((n_aux, n_act, 8, 128), BF16), pltpu.VMEM((n_act, width, width), F32)],
        flops=10**9,
    )
    summed = lax.all_to_all(shares, "aux", 0, 0, tiled=True)
    new_active, new_env = call(
        finish_kernel,
        [shape((n_act, rows_act, width), F32), shape((rows_env, n_env, width_env), F32)],
        [VMEM] * 4,
        summed, block, scale_act, scale_env,
    )
    return new_active, new_env.transpose(1, 0, 2)


def solution(mesh):
    rows = P("pair", "aux", None)
    deep = P("pair", None, "aux")
    per_pair = P("pair")
    level = (
        deep, deep, rows, per_pair, per_pair, P("pair", None),
        P("pair", None, None, None), P("pair", None), P("pair", None),
    )

    return jax.shard_map(
        shards, mesh=mesh, in_specs=level + level, out_specs=(rows, rows), check_vma=False
    )
```
